32 devices in a mesh: shard: 32 (over z, y, x, core).
Axes of the slice: x: 2, y: 2, z: 4, core: 2. Of those that a mesh axis runs over, the one named last changes fastest.
Arguments:
- lookup_ids: int32 [65536], P('shard'), may hold values from 0 to 524287, as said below
- grad_rows: float32 [65536, 128], P('shard'), may hold values from -6 to 6
- emb_table: float32 [524288, 128], P('shard'), may hold values from -4 to 4
- row_accum: float32 [524288], P('shard'), may hold values from 0.01 to 1
Outputs:
- new_table: float32 [524288, 128], P('shard')
- new_accum: float32 [524288], P('shard')
- looked_up: float32 [65536, 128], P('shard')
The draws below stay inside these ranges and needn't reach their ends.
Inputs may be any that keep to these rules, and one draw needn't show every extreme that they name: `lookup_ids`: each device's 2048 lookups name exactly 64 rows, repeats counted, in the range of every owner; within an owner's range the row numbers follow a power law, so that a few rows are named very often.
All inputs are finite; a program needn't handle non-finite values.
Results may differ from the reference program's by a relative error of at most 0.00002.
Values sent between devices are 32-bit elements; how exact they have to be, the bound alone decides.
A program may use at most 64 MiB of HBM per device.

```python
import math
import jax
import jax.numpy as jnp
from jax import lax

W = 128
ROWS_DEV = 16384
LOOK_DEV = 2048
ROWS = 524288
LOOKUPS = 65536
N_SHARD = 32


def draw_lookup_ids(key, part):
    key_perm, key_exp, key_row = jax.random.split(key, 3)
    perm_keys = jax.random.split(key_perm, N_SHARD)
    arrange = jax.vmap(lambda k: jax.random.permutation(k, LOOK_DEV))(perm_keys)
    owners = arrange % N_SHARD
    bit_count = ROWS_DEV.bit_length()
    exponent = jax.random.randint(key_exp, (N_SHARD, LOOK_DEV), 0, bit_count + 1)
    upper_limit = jnp.minimum(jnp.left_shift(jnp.ones_like(exponent), exponent), ROWS_DEV)
    local_rows = jax.random.randint(key_row, (N_SHARD, LOOK_DEV), 0, upper_limit)
    return (owners * ROWS_DEV + local_rows).reshape(-1).astype(jnp.int32)


def level_of(own_key, extent, cuts, low, largest):
    gain = 1.0
    for axis_at, parts in cuts:
        heights = jax.random.uniform(jax.random.fold_in(jax.random.fold_in(own_key, 6), axis_at), (parts,), jnp.float32, low / len(cuts), largest / len(cuts))
        gain = gain * jnp.repeat(jnp.exp(heights), extent[axis_at] // parts).reshape((-1,) + (1,) * (len(extent) - 1 - axis_at))
    return gain


def centred(own_key, dims, deviation, reach, shards=(), held_as=jnp.bfloat16):
    entries = deviation * jax.random.normal(own_key, dims, jnp.float32)
    if shards:
        entries = entries * level_of(own_key, dims, shards, -0.22, 0.18)
    return jnp.clip(entries, -reach, reach).astype(held_as)


def setup_inputs(seed: int = 0) -> dict:
    keys = jax.random.split(jax.random.key(seed), 5)
    return {
        "lookup_ids": draw_lookup_ids(jax.random.fold_in(keys[4], 71), 0),
        "grad_rows": centred(keys[1], (LOOKUPS, W), 1.0, 6.0, ((0, 32),), jnp.float32),
        "emb_table": centred(keys[2], (ROWS, W), 0.5, 4.0, ((0, 32),), jnp.float32),
        "row_accum": jnp.clip(jnp.exp(math.log(1.0) - 4.6051702 * jax.random.uniform(keys[3], (ROWS,), jnp.float32) ** level_of(keys[3], (ROWS,), ((0, 32),), -0.2, 0.2)), 0.01, 1.0),
    }


LEARNING_RATE = 0.5
EPSILON = 1e-08

def reference(lookup_ids, grad_rows, emb_table, row_accum):
    total_rows = emb_table.shape[0]
    summed = jax.ops.segment_sum(grad_rows, lookup_ids, num_segments=total_rows)
    new_accum = row_accum + lax.optimization_barrier(jnp.mean(summed * summed, axis=1))
    new_table = emb_table - LEARNING_RATE * summed / (jnp.sqrt(new_accum)[:, None] + EPSILON)
    looked_up = new_table[lookup_ids]
    return (new_table, new_accum, looked_up)
```

```python
import functools

import jax
import jax.numpy as jnp
from jax import lax
from jax.experimental import pallas as pl
from jax.experimental.pallas import tpu as pltpu
from jax.sharding import PartitionSpec as P

LEARNING_RATE = 0.5
EPSILON = 1e-08
LANES = 128
MIB = 1024 * 1024
F32 = jnp.float32
BF16 = jnp.bfloat16


def split3(x):
    hi = x.astype(BF16)
    rest = x - hi.astype(F32)
    mid = rest.astype(BF16)
    low = (rest - mid.astype(F32)).astype(BF16)
    return hi, mid, low


def dot(a, b):
    return jnp.dot(a, b, preferred_element_type=F32)


def column_of(row):
    return jnp.transpose(jnp.broadcast_to(row, (LANES, LANES)))


def one_hot_bf16(mask):
    return jnp.where(mask, 1.0, 0.0).astype(BF16)


def arrange_kernel(peers, rows_dev, ids_ref, grads_ref, pos_ref, send_ids_ref, send_ref, terms):
    blocks = ids_ref.shape[0]
    look = blocks * LANES
    per_peer = look // peers
    width = grads_ref.shape[1]
    peer_iota = lax.broadcasted_iota(jnp.int32, (peers, LANES), 0)
    before = one_hot_bf16(
        lax.broadcasted_iota(jnp.int32, (LANES, LANES), 0)
        < lax.broadcasted_iota(jnp.int32, (LANES, LANES), 1)
    )
    base = (per_peer * lax.broadcasted_iota(jnp.int32, (peers, 1), 0)).astype(F32)
    for b in range(blocks):
        ids = ids_ref[b : b + 1, :]
        owner = jnp.zeros_like(ids)
        low = peer_iota * rows_dev
        mine = jnp.where((ids >= low) & (ids < low + rows_dev), 1.0, 0.0)
        rank = dot(mine.astype(BF16), before) + base
        pos_ref[b : b + 1, :] = jnp.sum(mine * rank, axis=0, keepdims=True).astype(jnp.int32)
        base = base + jnp.sum(mine, axis=1, keepdims=True)
    hi, mid, low = split3(grads_ref[...])
    terms[:, 0:width] = hi
    terms[:, width : 2 * width] = mid
    terms[:, 2 * width : 3 * width] = low
    tile = 256
    pos = [pos_ref[b : b + 1, :] for b in range(blocks)]
    per_tile = tile // per_peer

    @pl.loop(0, look // tile)
    def _(t):
        start = pl.multiple_of(t * tile, tile)
        place = start + lax.broadcasted_iota(jnp.int32, (tile, LANES), 0)
        hits = [place == pos[b] for b in range(blocks)]
        pick = jnp.concatenate([one_hot_bf16(h) for h in hits], axis=1)
        out = dot(pick, terms[...])
        send_ref[pl.ds(start, tile), :] = (
            out[:, 0:width] + out[:, width : 2 * width] + out[:, 2 * width : 3 * width]
        )
        named = jnp.zeros((tile, LANES), jnp.int32)
        for b in range(blocks):
            named = named + jnp.where(hits[b], ids_ref[b : b + 1, :], 0)
        named = jnp.sum(named, axis=1, keepdims=True)
        slot = lax.rem(lax.broadcasted_iota(jnp.int32, (tile, LANES), 0), per_peer)
        lane = lax.broadcasted_iota(jnp.int32, (tile, LANES), 1)
        spread = jnp.where(slot == lane, jnp.broadcast_to(named, (tile, LANES)), 0)
        for q in range(per_tile):
            row = jnp.sum(spread[q * per_peer : (q + 1) * per_peer], axis=0, keepdims=True)
            peer = t * per_tile + q
            send_ids_ref[peer] = row - peer * rows_dev


def peer_of(me, step, n):
    return lax.rem(me + n // 2 + step, n)


def meet_all(me, n):
    barrier = pltpu.get_barrier_semaphore()

    def greet(step, carry):
        pl.semaphore_signal(
            barrier,
            inc=1,
            device_id=(lax.rem(me + step, n),),
            device_id_type=pl.DeviceIdType.MESH,
        )
        return carry

    lax.fori_loop(1, n, greet, 0)
    pl.semaphore_wait(barrier, n - 1)


def exchange_kernel(n, count, *refs):
    srcs, dsts = refs[:count], refs[count : 2 * count]
    send_sem, recv_sem, own_sem = refs[2 * count :]
    me = lax.axis_index("shard")
    own = [
        pltpu.make_async_copy(s.at[me], d.at[me], own_sem.at[i])
        for i, (s, d) in enumerate(zip(srcs, dsts))
    ]
    for copy in own:
        copy.start()
    meet_all(me, n)

    def remote(i, step):
        peer = lax.rem(me + step, n)
        return pltpu.make_async_remote_copy(
            src_ref=srcs[i].at[peer],
            dst_ref=dsts[i].at[me],
            send_sem=send_sem.at[i, step],
            recv_sem=recv_sem.at[i, step],
            device_id=(peer,),
            device_id_type=pl.DeviceIdType.MESH,
        )

    half = n // 2
    for i in range(count):

        def start(s, carry, i=i):
            remote(i, half + s).start()

            @pl.when(s > 0)
            def _():
                remote(i, half - s).start()

            return carry

        lax.fori_loop(0, half, start, 0)

    def finish(step, carry):
        for i in range(count):
            source = lax.rem(me - step + n, n)
            pltpu.make_async_remote_copy(
                src_ref=srcs[i].at[source],
                dst_ref=dsts[i].at[source],
                send_sem=send_sem.at[i, step],
                recv_sem=recv_sem.at[i, step],
                device_id=(source,),
                device_id_type=pl.DeviceIdType.MESH,
            ).wait_recv()
        return carry

    lax.fori_loop(1, n, finish, 0)

    def drain(step, carry):
        for i in range(count):
            remote(i, step).wait_send()
        return carry

    lax.fori_loop(1, n, drain, 0)
    for copy in own:
        copy.wait()


def exchange(n, collective_id, *arrays):
    count = len(arrays)
    vmem = pl.BlockSpec(memory_space=pltpu.VMEM)
    return pl.pallas_call(
        functools.partial(exchange_kernel, n, count),
        out_shape=[jax.ShapeDtypeStruct(a.shape, a.dtype) for a in arrays],
        in_specs=[vmem] * count,
        out_specs=[vmem] * count,
        scratch_shapes=[
            pltpu.SemaphoreType.DMA((count, n)),
            pltpu.SemaphoreType.DMA((count, n)),
            pltpu.SemaphoreType.DMA((count,)),
        ],
        compiler_params=pltpu.CompilerParams(
            collective_id=collective_id, has_side_effects=True, vmem_limit_bytes=16 * MIB
        ),
    )(*arrays)


def owner_kernel(
    ids_smem, ids_ref, grads_ref, accum_ref, emb_hbm,
    fresh_ref, new_accum_ref, table_hbm,
    table, terms, weights, hi_hot, lo_hot, in_sem, out_sem,
):
    blocks = ids_ref.shape[0]
    look = blocks * LANES
    width = grads_ref.shape[1]
    groups = accum_ref.shape[0]
    fetch = pltpu.make_async_copy(emb_hbm, table, in_sem)
    fetch.start()
    hi, mid, low = split3(grads_ref[...])
    terms[:, 0:width] = hi
    terms[:, width : 2 * width] = mid
    terms[:, 2 * width : 3 * width] = low
    terms[:, 3 * width : 4 * width] = jnp.ones((look, width), BF16)
    rows = [ids_ref[b : b + 1, :] for b in range(blocks)]
    acc3 = jnp.concatenate(split3(accum_ref[...]), axis=1)
    lane = lax.broadcasted_iota(jnp.int32, (LANES, LANES), 1)
    group_iota = lax.broadcasted_iota(jnp.int32, (LANES, groups), 1)
    fetch.wait()

    @pl.loop(0, blocks)
    def _(b):
        start = pl.multiple_of(b * LANES, LANES)
        here = pl.ds(start, LANES)
        col = column_of(ids_ref[pl.ds(b, 1), :])
        for i in range(LANES):
            fresh_ref[pl.ds(start + i, 1), :] = table[pl.ds(ids_smem[start + i], 1), :]
        same = jnp.concatenate([one_hot_bf16(col == r) for r in rows], axis=1)
        out = dot(same, terms[...])
        summed = out[:, 0:width] + out[:, width : 2 * width] + out[:, 2 * width : 3 * width]
        times = out[:, 3 * width : 3 * width + 1]
        mean = jnp.sum(summed * summed, axis=1, keepdims=True) * (1.0 / width)
        group = lax.shift_right_logical(col, 7)
        at_lane = (col & (LANES - 1)) == lane
        at_group = group[:, 0:1] == group_iota
        found = dot(one_hot_bf16(at_group), acc3)
        found = found[:, 0:LANES] + found[:, LANES : 2 * LANES] + found[:, 2 * LANES : 3 * LANES]
        acc = jnp.sum(jnp.where(at_lane, found, 0.0), axis=1, keepdims=True)
        new_acc = acc + mean
        fresh_ref[here, :] = fresh_ref[here, :] - LEARNING_RATE * summed / (
            jnp.sqrt(new_acc) + EPSILON
        )
        share = jnp.where(at_lane, jnp.broadcast_to(mean / times, (LANES, LANES)), 0.0)
        share_hi, share_mid, share_low = split3(share)
        weights[here, 0:LANES] = share_hi
        weights[here, LANES : 2 * LANES] = share_mid
        weights[here, 2 * LANES : 3 * LANES] = share_low
        hi_hot[here, :] = one_hot_bf16(at_group)

    @pl.loop(0, look // LANES)
    def _(b):
        start = pl.multiple_of(b * LANES, LANES)
        for i in range(LANES):
            table[pl.ds(ids_smem[start + i], 1), :] = fresh_ref[pl.ds(start + i, 1), :]

    store = pltpu.make_async_copy(table, table_hbm, out_sem)
    store.start()
    added = lax.dot_general(
        hi_hot[...], weights[...], (((0,), (0,)), ((), ())), preferred_element_type=F32
    )
    new_accum_ref[...] = accum_ref[...] + (
        added[:, 0:LANES] + added[:, LANES : 2 * LANES] + added[:, 2 * LANES : 3 * LANES]
    )
    store.wait()


def restore_kernel(pos_ref, back_ref, out_ref, terms):
    blocks = pos_ref.shape[0]
    width = back_ref.shape[1]
    hi, mid, low = split3(back_ref[...])
    terms[:, 0:width] = hi
    terms[:, width : 2 * width] = mid
    terms[:, 2 * width : 3 * width] = low
    lane = lax.broadcasted_iota(jnp.int32, (LANES, LANES), 1)

    @pl.loop(0, blocks)
    def _(b):
        col = column_of(pos_ref[pl.ds(b, 1), :])
        pick = jnp.concatenate(
            [one_hot_bf16(col == lane + k * LANES) for k in range(blocks)], axis=1
        )
        out = dot(pick, terms[...])
        out_ref[pl.ds(pl.multiple_of(b * LANES, LANES), LANES), :] = (
            out[:, 0:width] + out[:, width : 2 * width] + out[:, 2 * width : 3 * width]
        )


def on_device(lookup_ids, grad_rows, emb_table, row_accum):
    n = lax.axis_size("shard")
    look, width = grad_rows.shape
    rows_dev = emb_table.shape[0]
    per_peer = look // n
    blocks = look // LANES
    groups = rows_dev // LANES
    vmem = pl.BlockSpec(memory_space=pltpu.VMEM)
    smem = pl.BlockSpec(memory_space=pltpu.SMEM)
    anywhere = pl.BlockSpec(memory_space=pl.ANY)

    pos, send_ids, send = pl.pallas_call(
        functools.partial(arrange_kernel, n, rows_dev),
        out_shape=[
            jax.ShapeDtypeStruct((blocks, LANES), jnp.int32),
            jax.ShapeDtypeStruct((n, 1, LANES), jnp.int32),
            jax.ShapeDtypeStruct((look, width), F32),
        ],
        in_specs=[vmem, vmem],
        out_specs=[vmem] * 3,
        scratch_shapes=[pltpu.VMEM((look, 3 * width), BF16)],
        compiler_params=pltpu.CompilerParams(vmem_limit_bytes=24 * MIB),
    )(lookup_ids.reshape(blocks, LANES), grad_rows)

    recv_ids, recv = exchange(n, 1, send_ids, send.reshape(n, per_peer, width))
    local_ids = recv_ids[:, 0, :per_peer].reshape(look)

    fresh, new_accum, new_table = pl.pallas_call(
        owner_kernel,
        out_shape=[
            jax.ShapeDtypeStruct((look, width), F32),
            jax.ShapeDtypeStruct((groups, LANES), F32),
            jax.ShapeDtypeStruct((rows_dev, width), F32),
        ],
        in_specs=[smem, vmem, vmem, vmem, anywhere],
        out_specs=[vmem, vmem, anywhere],
        scratch_shapes=[
            pltpu.VMEM((rows_dev, width), F32),
            pltpu.VMEM((look, 4 * width), BF16),
            pltpu.VMEM((look, 3 * LANES), BF16),
            pltpu.VMEM((look, groups), BF16),
            pltpu.VMEM((8, LANES), BF16),
            pltpu.SemaphoreType.DMA(()),
            pltpu.SemaphoreType.DMA(()),
        ],
        compiler_params=pltpu.CompilerParams(vmem_limit_bytes=36 * MIB),
    )(
        local_ids,
        local_ids.reshape(blocks, LANES),
        recv.reshape(look, width),
        row_accum.reshape(groups, LANES),
        emb_table,
    )

    (back,) = exchange(n, 2, fresh.reshape(n, per_peer, width))

    looked_up = pl.pallas_call(
        restore_kernel,
        out_shape=jax.ShapeDtypeStruct((look, width), F32),
        in_specs=[vmem, vmem],
        out_specs=vmem,
        scratch_shapes=[pltpu.VMEM((look, 3 * width), BF16)],
        compiler_params=pltpu.CompilerParams(vmem_limit_bytes=24 * MIB),
    )(pos, back.reshape(look, width))
    return (new_table, new_accum.reshape(rows_dev), looked_up)


def solution(mesh):
    in_specs = (P("shard"), P("shard", None), P("shard", None), P("shard"))
    out_specs = (P("shard", None), P("shard"), P("shard", None))
    return jax.shard_map(
        on_device, mesh=mesh, in_specs=in_specs, out_specs=out_specs, check_vma=False
    )
```
